256 devices in a mesh: seq: 128 (over y, x_lo, z, core), dp: 2 (over x_hi).
Axes of the slice: x: 4 (x_hi: 2, x_lo: 2; x = x_hi * 2 + x_lo), y: 4, z: 8, core: 2. Of those that a mesh axis runs over, the one named last changes fastest.
Arguments:
- q_student: bfloat16 [2, 65536, 1536], P('dp', 'seq'), may hold values from -8 to 8
- kv_student: bfloat16 [2, 1024, 3072], P('dp', 'seq'), may hold values from -8 to 8
- q_target: bfloat16 [2, 65536, 1536], P('dp', 'seq'), may hold values from -8 to 8
- kv_target: bfloat16 [2, 1024, 3072], P('dp', 'seq'), may hold values from -8 to 8
Outputs:
- student_out: bfloat16 [2, 65536, 1536], P('dp', 'seq')
- target_out: bfloat16 [2, 65536, 1536], P('dp', 'seq')
- distill_loss: float32 [], replicated
The draws below stay inside these ranges and needn't reach their ends.
All inputs are finite; a program needn't handle non-finite values.
Results may differ from the reference program's by a relative error of at most 0.004.
Values may be sent and summed in bfloat16 or wider, within the bound.
A program may use at most 128 MiB of HBM per device.

```python
import jax
import jax.numpy as jnp
from jax import lax

HEADS = 12
HD = 128
TOK_DEV = 512
TOKENS = 65536
KV_TOKENS = 1024
CLIPS = 2
N_SEQ = 128


def draw_pairs(key, value_growth):
    feature_width = HEADS * HD
    key_list = jax.random.split(key, 7)
    clip_frac = jnp.arange(CLIPS).astype(jnp.float32)
    value_scale = 1.0 + value_growth * 1.5 * clip_frac
    queries = jnp.clip(2.5 * jax.random.normal(key_list[0], (CLIPS, TOKENS, feature_width), jnp.float32), -8.0, 8.0)
    key_part = jnp.clip(jax.random.normal(key_list[1], (CLIPS, KV_TOKENS, feature_width), jnp.float32), -6.0, 6.0)
    value_part = jnp.clip(jax.random.normal(key_list[6], (CLIPS, KV_TOKENS, feature_width), jnp.float32) * value_scale[:, None, None], -8.0, 8.0)
    key_values = jnp.concatenate([key_part, value_part], axis=2)
    return (queries, key_values)


def draw_q_student(key, part):
    return draw_pairs(jax.random.fold_in(key, 11), 0.0)[0].astype(jnp.bfloat16)


def draw_kv_student(key, part):
    return draw_pairs(jax.random.fold_in(key, 11), 0.0)[1].astype(jnp.bfloat16)


def draw_q_target(key, part):
    return draw_pairs(jax.random.fold_in(key, 23), 1.0)[0].astype(jnp.bfloat16)


def draw_kv_target(key, part):
    return draw_pairs(jax.random.fold_in(key, 23), 1.0)[1].astype(jnp.bfloat16)


def setup_inputs(seed: int = 0) -> dict:
    key_of = jax.random.split(jax.random.key(seed), 5)
    q_student = draw_q_student(jax.random.fold_in(key_of[4], 71), 0)
    kv_student = draw_kv_student(jax.random.fold_in(key_of[4], 71), 0)
    q_target = draw_q_target(jax.random.fold_in(key_of[4], 71), 0)
    kv_target = draw_kv_target(jax.random.fold_in(key_of[4], 71), 0)
    return dict(q_student=q_student, kv_student=kv_student, q_target=q_target, kv_target=kv_target)


def attend(queries, key_values):
    feature_width = HEADS * HD
    key_all = key_values[:, :feature_width].astype(jnp.float32).reshape(KV_TOKENS, HEADS, HD)
    value_all = key_values[:, feature_width:].astype(jnp.float32).reshape(KV_TOKENS, HEADS, HD)
    blocks = queries.reshape(N_SEQ, TOK_DEV, HEADS, HD)
    score_scale = 1.0 / (HD ** 0.5)

    def one_block(query_block):
        scores = jnp.einsum('qhd,khd->hqk', query_block.astype(jnp.float32), key_all) * score_scale
        row_max = jnp.max(scores, axis=-1, keepdims=True)
        exponent = jnp.exp(scores - row_max)
        row_total = jnp.sum(exponent, axis=-1)
        weights_bf = lax.optimization_barrier(exponent.astype(jnp.bfloat16)).astype(jnp.float32)
        mixed_rows = jnp.einsum('hqk,khd->hqd', weights_bf, value_all) / row_total[:, :, None]
        return jnp.transpose(mixed_rows, (1, 0, 2)).reshape(TOK_DEV, feature_width)

    return lax.map(one_block, blocks).reshape(TOKENS, feature_width)


def reference(q_student, kv_student, q_target, kv_target):
    student_rows = jnp.stack([attend(q_student[clip_index], kv_student[clip_index]) for clip_index in range(CLIPS)])
    target_rows = jnp.stack([attend(q_target[clip_index], kv_target[clip_index]) for clip_index in range(CLIPS)])
    position = jnp.arange(TOKENS).astype(jnp.float32)
    weight = 1.0 + 2.0 * position / float(max(TOKENS - 1, 1))
    gap_rows = student_rows - target_rows
    distill_loss = jnp.sum(weight[None, :, None] * gap_rows * gap_rows) / float(TOKENS * HEADS * HD)
    return student_rows.astype(jnp.bfloat16), target_rows.astype(jnp.bfloat16), distill_loss
```

```python
import functools
import heapq

import jax
import jax.numpy as jnp
from jax import lax
from jax.experimental import pallas as pl
from jax.experimental.pallas import tpu as pltpu
from jax.sharding import PartitionSpec as P

HEADS = 12
HD = 128
WIDTH = HEADS * HD
NY, NX, NZ = 4, 2, 8
SIZE = {"y": NY, "x": NX, "z": NZ}
AXIS = {"y": 0, "x": 1, "z": 2}
ROWS = 8
SLOTS = 2 * NY * NX * NZ
LINES = NY * NX
LOG2E = 1.4426950408889634
TREES = (("zyx", 0, 1536), ("zxy", 1536, 3840), ("yxz", 3840, 6144))


def signed(axis, v, d, salt):
    n = SIZE[axis]
    if axis == "x":
        return v
    if v * 2 == n:
        return v if (sum(d) - v + salt) % 2 == 0 else -v
    return v if v * 2 < n else v - n


def last_hop(order, d, salt):
    for axis in reversed(order):
        v = d[AXIS[axis]]
        if v:
            return axis, (1 if signed(axis, v, d, salt) > 0 else -1)
    return None


def children(order, d, salt):
    out = []
    for axis in "zyx":
        for s in (1, -1) if axis != "x" else (1,):
            nd = list(d)
            nd[AXIS[axis]] = (nd[AXIS[axis]] + s) % SIZE[axis]
            nd = tuple(nd)
            if nd != (0, 0, 0) and last_hop(order, nd, salt) == (axis, s):
                out.append((axis, s, nd))
    return out


def height(order, d, salt):
    return max([1 + height(order, c[2], salt) for c in children(order, d, salt)] or [0])


def relay_order():
    heap = [(0.0, k, k, (0, 0, 0)) for k in range(len(TREES))]
    count, free, core, order = len(TREES), {}, 0.0, []
    while heap:
        t, _, k, d = heapq.heappop(heap)
        name, lo, hi = TREES[k]
        core = max(core, t)
        kids = sorted(children(name, d, k), key=lambda c: -height(name, c[2], k))
        order.append((k, d, kids))
        for axis, s, nd in kids:
            core += 0.05
            end = max(core, free.get((axis, s), 0.0)) + (hi - lo) * 16 / 46.7e3
            free[(axis, s)] = end
            heapq.heappush(heap, (end + 1.9, count, k, nd))
            count += 1
    return order


def attend(q_ref, buf, col, head, kk, vv, rows):
    cols = pl.ds(pl.multiple_of(col + head * HD, HD), HD)
    vcols = pl.ds(pl.multiple_of(col + WIDTH + head * HD, HD), HD)
    key = buf[:, :, cols].astype(jnp.float32).reshape(SLOTS * ROWS, HD).astype(jnp.bfloat16)
    kk[:, :HD] = key
    kk[:, HD:] = key
    vv[:, :HD] = buf[:, :, vcols].astype(jnp.float32).reshape(SLOTS * ROWS, HD).astype(jnp.bfloat16)
    outs = []
    for r in range(0, q_ref.shape[0], rows):
        q = q_ref[r : r + rows, pl.ds(pl.multiple_of(head * HD, HD), HD)]
        scaled = q.astype(jnp.float32) * (LOG2E / HD**0.5)
        high = scaled.astype(jnp.bfloat16)
        low = (scaled - high.astype(jnp.float32)).astype(jnp.bfloat16)
        both = jnp.concatenate([high, low], axis=1)
        scores = lax.dot_general(both, kk[...], (((1,), (1,)), ((), ())), preferred_element_type=jnp.float32)
        expo = jnp.exp2(scores - jnp.max(scores, axis=1, keepdims=True)).astype(jnp.bfloat16)
        mixed = jnp.dot(expo, vv[...], preferred_element_type=jnp.float32)
        outs.append(mixed[:, :HD] / mixed[:, HD:])
    return outs


def kernel(
    qs_hbm, kvs_hbm, qt_hbm, kvt_hbm, os_hbm, ot_hbm, loss_ref,
    buf, qs, qt, outs, outt, kk, vv, acc,
    load_sem, q_sem, out_sem, ici_send, d2d_send, ici_recv, d2d_recv,
):
    seq = lax.axis_index("seq")
    core = lax.rem(seq, 2)
    z = lax.rem(seq // 2, NZ)
    x = lax.rem(seq // (2 * NZ), NX)
    y = seq // (2 * NZ * NX)

    def device(yy, xx, zz, cc):
        return {"seq": ((yy * NX + xx) * NZ + zz) * 2 + cc}

    def line(cc, yy, xx):
        return ((cc * NY + yy) * NX + xx) * NZ

    near = {
        ("z", 1): device(y, x, lax.rem(z + 1, NZ), core),
        ("z", -1): device(y, x, lax.rem(z + NZ - 1, NZ), core),
        ("y", 1): device(lax.rem(y + 1, NY), x, z, core),
        ("y", -1): device(lax.rem(y + NY - 1, NY), x, z, core),
        ("x", 1): device(y, 1 - x, z, core),
    }
    partner = device(y, x, z, 1 - core)
    ys = [lax.rem(y + NY - d, NY) for d in range(NY)]
    xs = [x, 1 - x]
    zs = [lax.rem(z + NZ - d, NZ) for d in range(NZ)]

    mine = line(core, y, x) + z
    load_s = pltpu.make_async_copy(kvs_hbm.at[0], buf.at[mine, :, : 2 * WIDTH], load_sem.at[0])
    load_t = pltpu.make_async_copy(kvt_hbm.at[0], buf.at[mine, :, 2 * WIDTH :], load_sem.at[1])
    load_s.start()
    load_t.start()
    barrier = pltpu.get_barrier_semaphore()
    for peer in list(near.values()) + [partner]:
        pl.semaphore_signal(barrier, inc=1, device_id=peer, device_id_type=pl.DeviceIdType.MESH)
    load_q = [
        pltpu.make_async_copy(qs_hbm.at[0], qs, q_sem.at[0]),
        pltpu.make_async_copy(qt_hbm.at[0], qt, q_sem.at[1]),
    ]
    for c in load_q:
        c.start()
    vv[:, HD:] = jnp.ones((SLOTS * ROWS, HD), jnp.bfloat16)
    acc[...] = jnp.zeros_like(acc)
    load_s.wait()
    load_t.wait()
    pl.semaphore_wait(barrier, 6)

    def remote(part, send, recv, to):
        return pltpu.make_async_remote_copy(
            src_ref=part, dst_ref=part, send_sem=send, recv_sem=recv,
            device_id=to, device_id_type=pl.DeviceIdType.MESH,
        )

    def item(k, d):
        _, lo, hi = TREES[k]
        return buf.at[line(core, ys[d[0]], xs[d[1]]) + zs[d[2]], :, lo:hi]

    def sem_of(k, d):
        return ici_recv.at[k, (d[0] * NX + d[1]) * NZ + d[2]]

    have = {}
    for k, d, kids in relay_order():
        _, lo, hi = TREES[k]
        if d != (0, 0, 0):
            remote(item(k, d), ici_send.at[k], sem_of(k, d), partner).wait_recv()
        for axis, s, nd in kids:
            remote(item(k, d), ici_send.at[k], sem_of(k, nd), near[(axis, s)]).start()
        spot = (k, d[0], d[1])
        have[spot] = have.get(spot, 0) + 1
        if have[spot] == NZ:
            part = buf.at[pl.ds(line(core, ys[d[0]], xs[d[1]]), NZ), :, lo:hi]
            remote(part, d2d_send.at[k], d2d_recv.at[k], partner).start()
    for k, (_, lo, hi) in enumerate(TREES):
        part = buf.at[pl.ds((1 - core) * LINES * NZ, LINES * NZ), :, lo:hi]
        remote(part, d2d_send.at[k], d2d_recv.at[k], partner).wait_recv()
    for c in load_q:
        c.wait()

    rows = qs.shape[0]
    block = 256

    def one_head(head, carry):
        a = attend(qs, buf, 0, head, kk, vv, block)
        b = attend(qt, buf, 2 * WIDTH, head, kk, vv, block)
        cols = pl.ds(pl.multiple_of(head * HD, HD), HD)
        for i, (s, t) in enumerate(zip(a, b)):
            at = pl.ds(i * block, block)
            outs[at, cols] = s.astype(jnp.bfloat16)
            outt[at, cols] = t.astype(jnp.bfloat16)
            gap = s - t
            acc[at, :] += gap * gap
        pltpu.make_async_copy(outs.at[:, cols], os_hbm.at[0, :, cols], out_sem.at[0]).start()
        pltpu.make_async_copy(outt.at[:, cols], ot_hbm.at[0, :, cols], out_sem.at[1]).start()
        return carry

    lax.fori_loop(0, HEADS, one_head, 0)

    spot = lax.broadcasted_iota(jnp.int32, (rows, HD), 0) + ((y * NX + x) * NZ + z) * 2 * rows + core * rows
    weight = 1.0 + 2.0 * spot.astype(jnp.float32) / float(rows * SLOTS - 1)
    loss_ref[...] = jnp.sum((weight * acc[...]).reshape(rows // 8, 8, HD), axis=0)

    for k, (_, lo, hi) in enumerate(TREES):
        part = buf.at[pl.ds(0, LINES * NZ - 1), :, lo:hi]
        remote(part, ici_send.at[k], d2d_recv.at[k], partner).wait_send()
        part = buf.at[pl.ds(0, LINES * NZ), :, lo:hi]
        remote(part, d2d_send.at[k], d2d_recv.at[k], partner).wait_send()
    pltpu.make_async_copy(outs, os_hbm.at[0], out_sem.at[0]).wait()
    pltpu.make_async_copy(outt, ot_hbm.at[0], out_sem.at[1]).wait()


def body(q_student, kv_student, q_target, kv_target):
    rows = q_student.shape[1]
    any_space = pl.BlockSpec(memory_space=pl.ANY)
    out = jax.ShapeDtypeStruct(q_student.shape, jnp.bfloat16)
    bf = jnp.bfloat16
    student, target, part = pl.pallas_call(
        kernel,
        out_shape=(out, out, jax.ShapeDtypeStruct((8, HD), jnp.float32)),
        in_specs=[any_space] * 4,
        out_specs=(any_space, any_space, pl.BlockSpec(memory_space=pltpu.VMEM)),
        scratch_shapes=[
            pltpu.VMEM((SLOTS, ROWS, 4 * WIDTH), bf),
            pltpu.VMEM((rows, WIDTH), bf),
            pltpu.VMEM((rows, WIDTH), bf),
            pltpu.VMEM((rows, WIDTH), bf),
            pltpu.VMEM((rows, WIDTH), bf),
            pltpu.VMEM((SLOTS * ROWS, 2 * HD), bf),
            pltpu.VMEM((SLOTS * ROWS, 2 * HD), bf),
            pltpu.VMEM((rows, HD), jnp.float32),
            pltpu.SemaphoreType.DMA((2,)),
            pltpu.SemaphoreType.DMA((2,)),
            pltpu.SemaphoreType.DMA((2,)),
            pltpu.SemaphoreType.DMA((len(TREES),)),
            pltpu.SemaphoreType.DMA((len(TREES),)),
            pltpu.SemaphoreType.DMA((len(TREES), LINES * NZ)),
            pltpu.SemaphoreType.DMA((len(TREES),)),
        ],
        compiler_params=pltpu.CompilerParams(
            collective_id=0, has_side_effects=True, vmem_limit_bytes=60 * 1024 * 1024
        ),
    )(q_student, kv_student, q_target, kv_target)
    total = jnp.sum(part) / float(2 * rows * SLOTS // 2 * WIDTH)
    return student, target, lax.psum(total, ("seq", "dp"))


def solution(mesh):
    spec = P("dp", "seq", None)
    return jax.shard_map(
        body, mesh=mesh, in_specs=(spec,) * 4, out_specs=(spec, spec, P()), check_vma=False
    )
```

```python
import functools
import heapq

import jax
import jax.numpy as jnp
from jax import lax
from jax.experimental import pallas as pl
from jax.experimental.pallas import tpu as pltpu
from jax.sharding import PartitionSpec as P

HEADS = 12
HD = 128
WIDTH = HEADS * HD
NY, NX, NZ = 4, 2, 8
SIZE = {"y": NY, "x": NX, "z": NZ}
AXIS = {"y": 0, "x": 1, "z": 2}
ROWS = 8
SLOTS = 2 * NY * NX * NZ
LINES = NY * NX
UNROLL = 4
LOG2E = 1.4426950408889634
TREES = (("zyx", 0, 1536), ("zxy", 1536, 3840), ("yxz", 3840, 6144))


def signed(axis, v, d, salt):
    n = SIZE[axis]
    if axis == "x":
        return v
    if v * 2 == n:
        return v if (sum(d) - v + salt) % 2 == 0 else -v
    return v if v * 2 < n else v - n


def last_hop(order, d, salt):
    for axis in reversed(order):
        v = d[AXIS[axis]]
        if v:
            return axis, (1 if signed(axis, v, d, salt) > 0 else -1)
    return None


def children(order, d, salt):
    out = []
    for axis in "zyx":
        for s in (1, -1) if axis != "x" else (1,):
            nd = list(d)
            nd[AXIS[axis]] = (nd[AXIS[axis]] + s) % SIZE[axis]
            nd = tuple(nd)
            if nd != (0, 0, 0) and last_hop(order, nd, salt) == (axis, s):
                out.append((axis, s, nd))
    return out


def height(order, d, salt):
    return max([1 + height(order, c[2], salt) for c in children(order, d, salt)] or [0])


def relay_order():
    heap = [(0.0, k, k, (0, 0, 0)) for k in range(len(TREES))]
    count, free, core, order = len(TREES), {}, 0.0, []
    while heap:
        t, _, k, d = heapq.heappop(heap)
        name, lo, hi = TREES[k]
        core = max(core, t)
        kids = sorted(children(name, d, k), key=lambda c: -height(name, c[2], k))
        order.append((k, d, kids))
        for axis, s, nd in kids:
            core += 0.05
            end = max(core, free.get((axis, s), 0.0)) + (hi - lo) * 16 / 46.7e3
            free[(axis, s)] = end
            heapq.heappush(heap, (end + 1.9, count, k, nd))
            count += 1
    return order


def attend(q_ref, buf, col, head, kk, vv, rows):
    cols = pl.ds(pl.multiple_of(col + head * HD, HD), HD)
    vcols = pl.ds(pl.multiple_of(col + WIDTH + head * HD, HD), HD)
    kk[...] = buf[:, :, cols].astype(jnp.float32).reshape(SLOTS * ROWS, HD).astype(jnp.bfloat16)
    vv[:, :HD] = buf[:, :, vcols].astype(jnp.float32).reshape(SLOTS * ROWS, HD).astype(jnp.bfloat16)
    outs = []
    for r in range(0, q_ref.shape[0], rows):
        q = q_ref[r : r + rows, pl.ds(pl.multiple_of(head * HD, HD), HD)]
        scores = lax.dot_general(q, kk[...], (((1,), (1,)), ((), ())), preferred_element_type=jnp.float32)
        scores = (scores - jnp.max(scores, axis=1, keepdims=True)) * (LOG2E / HD**0.5)
        expo = jnp.exp2(scores).astype(jnp.bfloat16)
        mixed = jnp.dot(expo, vv[...], preferred_element_type=jnp.float32)
        outs.append(mixed[:, :HD] / mixed[:, HD:])
    return outs


def kernel(
    qs_hbm, kvs_hbm, qt_hbm, kvt_hbm, os_hbm, ot_hbm, loss_ref,
    buf, qs, qt, outs, outt, kk, vv, acc,
    total_in, total_out, load_sem, q_sem, out_sem, ici_send, d2d_send, ici_recv, d2d_recv, sum_send, sum_recv,
):
    seq = lax.axis_index("seq")
    dp = lax.axis_index("dp")
    core = lax.rem(seq, 2)
    z = lax.rem(seq // 2, NZ)
    x = lax.rem(seq // (2 * NZ), NX)
    y = seq // (2 * NZ * NX)

    def device(yy, xx, zz, cc, dd=dp):
        return {"seq": ((yy * NX + xx) * NZ + zz) * 2 + cc, "dp": dd}

    def line(cc, yy, xx):
        return ((cc * NY + yy) * NX + xx) * NZ

    near = {
        ("z", 1): device(y, x, lax.rem(z + 1, NZ), core),
        ("z", -1): device(y, x, lax.rem(z + NZ - 1, NZ), core),
        ("y", 1): device(lax.rem(y + 1, NY), x, z, core),
        ("y", -1): device(lax.rem(y + NY - 1, NY), x, z, core),
        ("x", 1): device(y, 1 - x, z, core),
    }
    partner = device(y, x, z, 1 - core)
    ys = [lax.rem(y + NY - d, NY) for d in range(NY)]
    xs = [x, 1 - x]
    zs = [lax.rem(z + NZ - d, NZ) for d in range(NZ)]

    cube = []
    for i in range(1, 8):
        cube.append(device(y, lax.rem(x + i // 4, 2), z, lax.rem(core + i // 2 % 2, 2), lax.rem(dp + i % 2, 2)))
    sums = (
        ((x * 2 + core) * 2 + dp, cube),
        (y, [device(lax.rem(y + i, NY), x, z, core) for i in range(1, NY)]),
        (z, [device(y, x, lax.rem(z + i, NZ), core) for i in range(1, NZ)]),
    )
    peers = [p for _, group in sums for p in group]

    mine = line(core, y, x) + z
    load_s = pltpu.make_async_copy(kvs_hbm.at[0], buf.at[mine, :, : 2 * WIDTH], load_sem.at[0])
    load_t = pltpu.make_async_copy(kvt_hbm.at[0], buf.at[mine, :, 2 * WIDTH :], load_sem.at[1])
    load_s.start()
    load_t.start()
    barrier = pltpu.get_barrier_semaphore()
    for peer in peers:
        pl.semaphore_signal(barrier, inc=1, device_id=peer, device_id_type=pl.DeviceIdType.MESH)
    load_q = [
        pltpu.make_async_copy(qs_hbm.at[0], qs, q_sem.at[0]),
        pltpu.make_async_copy(qt_hbm.at[0], qt, q_sem.at[1]),
    ]
    for c in load_q:
        c.start()
    vv[:, :, :, HD:] = jnp.ones((UNROLL, 2, SLOTS * ROWS, HD), jnp.bfloat16)
    acc[...] = jnp.zeros_like(acc)
    load_s.wait()
    load_t.wait()
    pl.semaphore_wait(barrier, len(peers))

    def remote(part, send, recv, to):
        return pltpu.make_async_remote_copy(
            src_ref=part, dst_ref=part, send_sem=send, recv_sem=recv,
            device_id=to, device_id_type=pl.DeviceIdType.MESH,
        )

    def item(k, d):
        _, lo, hi = TREES[k]
        return buf.at[line(core, ys[d[0]], xs[d[1]]) + zs[d[2]], :, lo:hi]

    def sem_of(k, d):
        return ici_recv.at[k, (d[0] * NX + d[1]) * NZ + d[2]]

    have = {}
    for k, d, kids in relay_order():
        _, lo, hi = TREES[k]
        if d != (0, 0, 0):
            remote(item(k, d), ici_send.at[k], sem_of(k, d), partner).wait_recv()
        for axis, s, nd in kids:
            remote(item(k, d), ici_send.at[k], sem_of(k, nd), near[(axis, s)]).start()
        spot = (k, d[0], d[1])
        have[spot] = have.get(spot, 0) + 1
        if have[spot] == NZ:
            part = buf.at[pl.ds(line(core, ys[d[0]], xs[d[1]]), NZ), :, lo:hi]
            remote(part, d2d_send.at[k], d2d_recv.at[k], partner).start()
    for k, (_, lo, hi) in enumerate(TREES):
        part = buf.at[pl.ds((1 - core) * LINES * NZ, LINES * NZ), :, lo:hi]
        remote(part, d2d_send.at[k], d2d_recv.at[k], partner).wait_recv()
    for c in load_q:
        c.wait()

    rows = qs.shape[0]
    block = 256

    def some_heads(step, carry):
        for u in range(UNROLL):
            head = step * UNROLL + u
            a = attend(qs, buf, 0, head, kk.at[u, 0], vv.at[u, 0], block)
            b = attend(qt, buf, 2 * WIDTH, head, kk.at[u, 1], vv.at[u, 1], block)
            cols = pl.ds(pl.multiple_of(head * HD, HD), HD)
            for i, (s, t) in enumerate(zip(a, b)):
                at = pl.ds(i * block, block)
                outs[at, cols] = s.astype(jnp.bfloat16)
                outt[at, cols] = t.astype(jnp.bfloat16)
                gap = s - t
                acc[at, :] += gap * gap
        cols = pl.ds(pl.multiple_of(step * (UNROLL * HD), HD), UNROLL * HD)
        pltpu.make_async_copy(outs.at[:, cols], os_hbm.at[0, :, cols], out_sem.at[0]).start()
        pltpu.make_async_copy(outt.at[:, cols], ot_hbm.at[0, :, cols], out_sem.at[1]).start()
        return carry

    lax.fori_loop(0, HEADS // UNROLL, some_heads, 0)

    spot = lax.broadcasted_iota(jnp.int32, (rows, HD), 0) + ((y * NX + x) * NZ + z) * 2 * rows + core * rows
    weight = 1.0 + 2.0 * spot.astype(jnp.float32) / float(rows * SLOTS - 1)
    total = jnp.sum((weight * acc[...]).reshape(rows // 8, 8, HD), axis=0)
    for i, (spot, group) in enumerate(sums):
        total_out[i] = total
        total_in[i, spot] = total
        for to in group:
            pltpu.make_async_remote_copy(
                src_ref=total_out.at[i], dst_ref=total_in.at[i, spot], send_sem=sum_send.at[i],
                recv_sem=sum_recv.at[i], device_id=to, device_id_type=pl.DeviceIdType.MESH,
            ).start()
        every = total_in.at[i, pl.ds(0, len(group))]
        remote(every, sum_send.at[i], sum_recv.at[i], partner).wait()
        total = jnp.sum(total_in[i, : len(group) + 1], axis=0)
    loss_ref[0, 0] = jnp.sum(total) / float(rows * SLOTS * WIDTH)

    for k, (_, lo, hi) in enumerate(TREES):
        part = buf.at[pl.ds(0, LINES * NZ - 1), :, lo:hi]
        remote(part, ici_send.at[k], d2d_recv.at[k], partner).wait_send()
        part = buf.at[pl.ds(0, LINES * NZ), :, lo:hi]
        remote(part, d2d_send.at[k], d2d_recv.at[k], partner).wait_send()
    pltpu.make_async_copy(outs, os_hbm.at[0], out_sem.at[0]).wait()
    pltpu.make_async_copy(outt, ot_hbm.at[0], out_sem.at[1]).wait()


def body(q_student, kv_student, q_target, kv_target):
    rows = q_student.shape[1]
    any_space = pl.BlockSpec(memory_space=pl.ANY)
    out = jax.ShapeDtypeStruct(q_student.shape, jnp.bfloat16)
    bf = jnp.bfloat16
    student, target, part = pl.pallas_call(
        kernel,
        out_shape=(out, out, jax.ShapeDtypeStruct((1, 1), jnp.float32)),
        in_specs=[any_space] * 4,
        out_specs=(any_space, any_space, pl.BlockSpec(memory_space=pltpu.SMEM)),
        scratch_shapes=[
            pltpu.VMEM((SLOTS, ROWS, 4 * WIDTH), bf),
            pltpu.VMEM((rows, WIDTH), bf),
            pltpu.VMEM((rows, WIDTH), bf),
            pltpu.VMEM((rows, WIDTH), bf),
            pltpu.VMEM((rows, WIDTH), bf),
            pltpu.VMEM((UNROLL, 2, SLOTS * ROWS, HD), bf),
            pltpu.VMEM((UNROLL, 2, SLOTS * ROWS, 2 * HD), bf),
            pltpu.VMEM((rows, HD), jnp.float32),
            pltpu.VMEM((3, 8, 8, HD), jnp.float32),
            pltpu.VMEM((3, 8, HD), jnp.float32),
            pltpu.SemaphoreType.DMA((2,)),
            pltpu.SemaphoreType.DMA((2,)),
            pltpu.SemaphoreType.DMA((2,)),
            pltpu.SemaphoreType.DMA((len(TREES),)),
            pltpu.SemaphoreType.DMA((len(TREES),)),
            pltpu.SemaphoreType.DMA((len(TREES), LINES * NZ)),
            pltpu.SemaphoreType.DMA((len(TREES),)),
            pltpu.SemaphoreType.DMA((3,)),
            pltpu.SemaphoreType.DMA((3,)),
        ],
        compiler_params=pltpu.CompilerParams(
            collective_id=0, has_side_effects=True, vmem_limit_bytes=60 * 1024 * 1024
        ),
    )(q_student, kv_student, q_target, kv_target)
    return student, target, part[0, 0]


def solution(mesh):
    spec = P("dp", "seq", None)
    return jax.shard_map(
        body, mesh=mesh, in_specs=(spec,) * 4, out_specs=(spec, spec, P()), check_vma=False
    )
```

```python
import functools
import heapq

import jax
import jax.numpy as jnp
from jax import lax
from jax.experimental import pallas as pl
from jax.experimental.pallas import tpu as pltpu
from jax.sharding import PartitionSpec as P

HEADS = 12
HD = 128
WIDTH = HEADS * HD
NY, NX, NZ = 4, 2, 8
SIZE = {"y": NY, "x": NX, "z": NZ}
AXIS = {"y": 0, "x": 1, "z": 2}
ROWS = 8
SLOTS = 2 * NY * NX * NZ
LINES = NY * NX
LOG2E = 1.4426950408889634
UNITS = 2 * HEADS
GROUPS = (
    ("yxz", 0, 4, 9.0, 2, 0),
    ("zxy", 0, 4, 1.0, 1, 1),
    ("yxz", 0, 3, 0.0, 1, 2),
    ("zxy", 1, 3, 0.0, 0, 2),
    ("zxy", 0, 5, 12.0, 1, 1),
    ("yzx", 1, 5, 1.0, 2, 0),
)
LATENCY = 3.0
FIRST = [sum(g[2] for g in GROUPS[:i]) for i in range(len(GROUPS))]
KEEP = 3


def signed(axis, v, d, salt):
    n = SIZE[axis]
    if axis == "x":
        return v
    if v * 2 == n:
        return v if (sum(d) - v + salt) % 2 == 0 else -v
    return v if v * 2 < n else v - n


def children(order, d, salt, jump):
    out = []
    for axis in "zyx":
        for s in (2, -2, 1, -1) if axis != "x" else (1,):
            nd = list(d)
            nd[AXIS[axis]] = (nd[AXIS[axis]] + s) % SIZE[axis]
            nd = tuple(nd)
            if nd == (0, 0, 0) or axis != next(a for a in reversed(order) if nd[AXIS[a]]):
                continue
            v = signed(axis, nd[AXIS[axis]], nd, salt)
            step = 2 if v % 2 == 0 and order.index(axis) < jump else 1
            if s == (step if v > 0 else -step):
                out.append((axis, s, nd))
    return out


def height(order, d, salt, jump):
    return max([1 + height(order, c[2], salt, jump) for c in children(order, d, salt, jump)] or [0])


def plan():
    pend, ready, free, log, count, now, held = [], [], {}, [], 0, 0.0, False
    got, done, left = [0] * len(GROUPS), [None] * len(GROUPS), [g[2] for g in GROUPS]
    for k, g in enumerate(GROUPS):
        heapq.heappush(pend, (g[3], count, k, (0, 0, 0)))
        count += 1
    while pend or ready or any(left) or held:
        while pend and pend[0][0] <= now:
            at, _, k, d = heapq.heappop(pend)
            name, salt, _, _, rank, jump = GROUPS[k]
            heapq.heappush(ready, ((rank, -height(name, d, salt, jump), at), k, d))
        if ready:
            _, k, d = heapq.heappop(ready)
            name, salt, units, _, _, jump = GROUPS[k]
            kids = sorted(children(name, d, salt, jump), key=lambda c: -height(name, c[2], salt, jump))
            log.append(("relay", k, d, kids))
            now += 0.016
            for axis, s, nd in kids:
                now += 0.016
                way = (axis, s > 0)
                busy = units * 4096 / 46.7e3
                start = max(now, free.get(way, 0.0))
                free[way] = start + abs(s) * busy
                heapq.heappush(pend, (start + busy + LATENCY + 0.8 * (abs(s) - 1), count, k, nd))
                count += 1
            got[k] += 1
            if got[k] == NY * NX * NZ:
                done[k] = now + 1.6
            continue
        open_groups = [k for k in range(len(GROUPS)) if left[k] and done[k] is not None]
        best = min(open_groups, key=lambda k: done[k], default=None)
        if best is not None and done[best] <= now:
            log.append(("unit", best, GROUPS[best][2] - left[best]))
            left[best] -= 1
            now += 0.7 if held else 0.4
            held = True
            continue
        later = min([p[0] for p in pend[:1]] + [done[k] for k in open_groups], default=now + 9)
        if held and later > now + 0.3:
            log.append(("flush",))
            now += 0.55
            held = False
            continue
        now = later
    return log


def score(q, buf, unit, kk, scores):
    keys = SLOTS * ROWS
    kk[...] = buf[:, 2 * unit].astype(jnp.float32).reshape(keys, HD).astype(jnp.bfloat16)
    for at in range(0, keys, 256):
        scores[:, at : at + 256] = lax.dot_general(
            q, kk[at : at + 256], (((1,), (1,)), ((), ())), preferred_element_type=jnp.float32
        )


def mix(buf, unit, vv, scores, block):
    vv[:, :HD] = buf[:, 2 * unit + 1].astype(jnp.float32).reshape(SLOTS * ROWS, HD).astype(jnp.bfloat16)
    outs = []
    for r in range(0, scores.shape[0], block):
        part = scores[r : r + block]
        part = (part - jnp.max(part, axis=1, keepdims=True)) * (LOG2E / HD**0.5)
        expo = jnp.exp2(part).astype(jnp.bfloat16)
        mixed = jnp.dot(expo, vv[...], preferred_element_type=jnp.float32)
        outs.append(mixed[:, :HD] / mixed[:, HD:])
    return outs


def kernel(
    qs_hbm, kvs_hbm, qt_hbm, kvt_hbm, outs, outt, loss_ref,
    buf, qs, qt, kk, vv, scores, other, acc,
    total_in, total_out, load_sem, q_sem, ici_send, d2d_send, ici_recv, d2d_recv, sum_send, sum_recv,
):
    seq = lax.axis_index("seq")
    dp = lax.axis_index("dp")
    core = lax.rem(seq, 2)
    z = lax.rem(seq // 2, NZ)
    x = lax.rem(seq // (2 * NZ), NX)
    y = seq // (2 * NZ * NX)

    def device(yy, xx, zz, cc, dd=dp):
        return {"seq": ((yy * NX + xx) * NZ + zz) * 2 + cc, "dp": dd}

    def line(cc, yy, xx):
        return ((cc * NY + yy) * NX + xx) * NZ

    near = {
        ("z", 1): device(y, x, lax.rem(z + 1, NZ), core),
        ("z", -1): device(y, x, lax.rem(z + NZ - 1, NZ), core),
        ("z", 2): device(y, x, lax.rem(z + 2, NZ), core),
        ("z", -2): device(y, x, lax.rem(z + NZ - 2, NZ), core),
        ("y", 1): device(lax.rem(y + 1, NY), x, z, core),
        ("y", -1): device(lax.rem(y + NY - 1, NY), x, z, core),
        ("y", 2): device(lax.rem(y + 2, NY), x, z, core),
        ("y", -2): device(lax.rem(y + 2, NY), x, z, core),
        ("x", 1): device(y, 1 - x, z, core),
    }
    partner = device(y, x, z, 1 - core)
    ys = [lax.rem(y + NY - d, NY) for d in range(NY)]
    xs = [x, 1 - x]
    zs = [lax.rem(z + NZ - d, NZ) for d in range(NZ)]

    cube = []
    for i in range(1, 8):
        cube.append(device(y, lax.rem(x + i // 4, 2), z, lax.rem(core + i // 2 % 2, 2), lax.rem(dp + i % 2, 2)))
    plane = [
        device(lax.rem(y + i // NZ, NY), x, lax.rem(z + i % NZ, NZ), core) for i in range(1, NY * NZ)
    ]
    sums = ((y * NZ + z, plane), ((x * 2 + core) * 2 + dp, cube))
    peers = [to for way, to in near.items() if way not in (("y", -2), ("x", 1))] + cube

    mine = line(core, y, x) + z
    barrier = pltpu.get_barrier_semaphore()
    for peer in peers:
        pl.semaphore_signal(barrier, inc=1, device_id=peer, device_id_type=pl.DeviceIdType.MESH)
    for unit in range(UNITS):
        head, kv = unit // 2, (kvs_hbm, kvt_hbm)[unit % 2]
        for part in range(2):
            cols = pl.ds(part * WIDTH + head * HD, HD)
            pltpu.make_async_copy(kv.at[0, :, cols], buf.at[mine, 2 * unit + part], load_sem.at[0]).start()
    load_q = [
        pltpu.make_async_copy(qs_hbm.at[0], qs, q_sem.at[0]),
        pltpu.make_async_copy(qt_hbm.at[0], qt, q_sem.at[1]),
    ]
    for c in load_q:
        c.start()
    vv[:, :, HD:] = jnp.ones((KEEP, SLOTS * ROWS, HD), jnp.bfloat16)
    acc[...] = jnp.zeros_like(acc)
    pltpu.make_async_copy(buf.at[mine], buf.at[mine], load_sem.at[0]).wait()
    pl.semaphore_wait(barrier, len(peers))

    def remote(part, send, recv, to):
        return pltpu.make_async_remote_copy(
            src_ref=part, dst_ref=part, send_sem=send, recv_sem=recv,
            device_id=to, device_id_type=pl.DeviceIdType.MESH,
        )

    def cut(k):
        return pl.ds(2 * FIRST[k], 2 * GROUPS[k][2])

    def item(k, d):
        return buf.at[line(core, ys[d[0]], xs[d[1]]) + zs[d[2]], cut(k)]

    def sem_of(k, d):
        return ici_recv.at[k, (d[0] * NX + d[1]) * NZ + d[2]]

    rows = qs.shape[0]
    block = 256
    have, ran, seen, loaded = {}, 0, set(), False

    def finish(unit, slot):
        head, model = unit // 2, unit % 2
        cols = slice(head * HD, head * HD + HD)
        for i, r in enumerate(mix(buf, unit, vv.at[slot], scores.at[slot], block)):
            at = slice(i * block, i * block + block)
            (outs, outt)[model][0, at, cols] = r.astype(jnp.bfloat16)
            if head in seen:
                gap = other[head, at, :] - r
                acc[at, :] += gap * gap
            else:
                other[head, at, :] = r
        seen.add(head)

    held = None
    for kind, *what in plan():
        if kind == "flush":
            finish(*held)
            held = None
            continue
        if kind == "unit":
            k, d = what
            if not loaded:
                for c in load_q:
                    c.wait()
                loaded = True
            if d == 0:
                part = buf.at[pl.ds((1 - core) * LINES * NZ, LINES * NZ), cut(k)]
                remote(part, d2d_send.at[k], d2d_recv.at[k], partner).wait_recv()
            unit = FIRST[k] + d
            slot = ran % KEEP
            ran += 1
            score((qs, qt)[unit % 2][:, unit // 2 * HD : unit // 2 * HD + HD], buf, unit, kk.at[slot], scores.at[slot])
            if held:
                finish(*held)
            held = (unit, slot)
            continue
        k, d, kids = what
        if d != (0, 0, 0):
            remote(item(k, d), ici_send.at[k], sem_of(k, d), partner).wait_recv()
        for axis, s, nd in kids:
            remote(item(k, d), ici_send.at[k], sem_of(k, nd), near[(axis, s)]).start()
        spot = (k, d[0], d[1])
        have[spot] = have.get(spot, 0) + 1
        if have[spot] == NZ:
            part = buf.at[pl.ds(line(core, ys[d[0]], xs[d[1]]), NZ), cut(k)]
            remote(part, d2d_send.at[k], d2d_recv.at[k], partner).start()

    spot = lax.broadcasted_iota(jnp.int32, (rows, HD), 0) + ((y * NX + x) * NZ + z) * 2 * rows + core * rows
    weight = 1.0 + 2.0 * spot.astype(jnp.float32) / float(rows * SLOTS - 1)
    total = jnp.sum((weight * acc[...]).reshape(rows // 8, 8, HD), axis=0)
    for i, (spot, group) in enumerate(sums):
        total_out[i] = total
        total_in[i, spot] = total
        for to in group:
            pltpu.make_async_remote_copy(
                src_ref=total_out.at[i], dst_ref=total_in.at[i, spot], send_sem=sum_send.at[i],
                recv_sem=sum_recv.at[i], device_id=to, device_id_type=pl.DeviceIdType.MESH,
            ).start()
        every = total_in.at[i, pl.ds(0, len(group))]
        remote(every, sum_send.at[i], sum_recv.at[i], partner).wait()
        total = jnp.sum(total_in[i, : len(group) + 1], axis=0)
    loss_ref[...] = total

    for k in range(len(GROUPS)):
        part = buf.at[pl.ds(0, LINES * NZ - 1), cut(k)]
        remote(part, ici_send.at[k], d2d_recv.at[k], partner).wait_send()
        part = buf.at[pl.ds(0, LINES * NZ), cut(k)]
        remote(part, d2d_send.at[k], d2d_recv.at[k], partner).wait_send()


def write(count, s_ref, t_ref, total_ref, os_hbm, ot_hbm, loss_ref, sem):
    copies = [
        pltpu.make_async_copy(s_ref, os_hbm, sem.at[0]),
        pltpu.make_async_copy(t_ref, ot_hbm, sem.at[1]),
    ]
    for c in copies:
        c.start()
    loss_ref[0] = jnp.sum(total_ref[...]) / count
    for c in copies:
        c.wait()


def body(q_student, kv_student, q_target, kv_target):
    rows = q_student.shape[1]
    bf = jnp.bfloat16
    any_space = pl.BlockSpec(memory_space=pl.ANY)
    vmem = pl.BlockSpec(memory_space=pltpu.VMEM)
    student, target, total = pl.pallas_call(
        kernel,
        out_shape=(
            pltpu.VMEM(q_student.shape, bf),
            pltpu.VMEM(q_student.shape, bf),
            pltpu.VMEM((8, HD), jnp.float32),
        ),
        in_specs=[any_space] * 4,
        out_specs=(vmem,) * 3,
        scratch_shapes=[
            pltpu.VMEM((SLOTS, 2 * UNITS, ROWS, HD), bf),
            pltpu.VMEM((rows, WIDTH), bf),
            pltpu.VMEM((rows, WIDTH), bf),
            pltpu.VMEM((KEEP, SLOTS * ROWS, HD), bf),
            pltpu.VMEM((KEEP, SLOTS * ROWS, 2 * HD), bf),
            pltpu.VMEM((KEEP, rows, SLOTS * ROWS), jnp.float32),
            pltpu.VMEM((HEADS, rows, HD), jnp.float32),
            pltpu.VMEM((rows, HD), jnp.float32),
            pltpu.VMEM((2, NY * NZ, 8, HD), jnp.float32),
            pltpu.VMEM((2, 8, HD), jnp.float32),
            pltpu.SemaphoreType.DMA((1,)),
            pltpu.SemaphoreType.DMA((2,)),
            pltpu.SemaphoreType.DMA((len(GROUPS),)),
            pltpu.SemaphoreType.DMA((len(GROUPS),)),
            pltpu.SemaphoreType.DMA((len(GROUPS), LINES * NZ)),
            pltpu.SemaphoreType.DMA((len(GROUPS),)),
            pltpu.SemaphoreType.DMA((2,)),
            pltpu.SemaphoreType.DMA((2,)),
        ],
        compiler_params=pltpu.CompilerParams(
            collective_id=0, has_side_effects=True, vmem_limit_bytes=52 * 1024 * 1024
        ),
    )(q_student, kv_student, q_target, kv_target)
    student, target, loss = pl.pallas_call(
        functools.partial(write, float(rows * SLOTS * WIDTH)),
        out_shape=(
            jax.ShapeDtypeStruct(q_student.shape, bf),
            jax.ShapeDtypeStruct(q_student.shape, bf),
            jax.ShapeDtypeStruct((1,), jnp.float32),
        ),
        in_specs=[vmem] * 3,
        out_specs=(any_space, any_space, pl.BlockSpec(memory_space=pltpu.SMEM)),
        scratch_shapes=[pltpu.SemaphoreType.DMA((2,))],
        compiler_params=pltpu.CompilerParams(vmem_limit_bytes=16 * 1024 * 1024),
    )(student, target, total)
    return student, target, loss.reshape(())


def solution(mesh):
    spec = P("dp", "seq", None)
    return jax.shard_map(
        body, mesh=mesh, in_specs=(spec,) * 4, out_specs=(spec, spec, P()), check_vma=False
    )
```

```python
import functools
import heapq

import jax
import jax.numpy as jnp
from jax import lax
from jax.experimental import pallas as pl
from jax.experimental.pallas import tpu as pltpu
from jax.sharding import PartitionSpec as P

HEADS = 12
HD = 128
WIDTH = HEADS * HD
NY, NX, NZ = 4, 2, 8
SIZE = {"y": NY, "x": NX, "z": NZ}
AXIS = {"y": 0, "x": 1, "z": 2}
ROWS = 8
SLOTS = 2 * NY * NX * NZ
LINES = NY * NX
LOG2E = 1.4426950408889634
UNITS = 2 * HEADS
GROUPS = (
    ("yxz", 0, 4, 9.0, 2, 0),
    ("zxy", 0, 4, 1.0, 1, 1),
    ("yxz", 0, 3, 0.0, 1, 2),
    ("zxy", 1, 3, 0.0, 0, 2),
    ("zxy", 0, 5, 12.0, 1, 1),
    ("yzx", 1, 5, 1.0, 2, 0),
)
LATENCY = 3.0
FIRST = [sum(g[2] for g in GROUPS[:i]) for i in range(len(GROUPS))]
KEEP = 3


def signed(axis, v, d, salt):
    n = SIZE[axis]
    if axis == "x":
        return v
    if v * 2 == n:
        return v if (sum(d) - v + salt) % 2 == 0 else -v
    return v if v * 2 < n else v - n


def children(order, d, salt, jump):
    out = []
    for axis in "zyx":
        for s in (2, -2, 1, -1) if axis != "x" else (1,):
            nd = list(d)
            nd[AXIS[axis]] = (nd[AXIS[axis]] + s) % SIZE[axis]
            nd = tuple(nd)
            if nd == (0, 0, 0) or axis != next(a for a in reversed(order) if nd[AXIS[a]]):
                continue
            v = signed(axis, nd[AXIS[axis]], nd, salt)
            step = 2 if v % 2 == 0 and order.index(axis) < jump else 1
            if s == (step if v > 0 else -step):
                out.append((axis, s, nd))
    return out


def height(order, d, salt, jump):
    return max([1 + height(order, c[2], salt, jump) for c in children(order, d, salt, jump)] or [0])


def plan():
    pend, ready, free, log, count, now, held = [], [], {}, [], 0, 0.0, False
    got, done, left = [0] * len(GROUPS), [None] * len(GROUPS), [g[2] for g in GROUPS]
    for k, g in enumerate(GROUPS):
        heapq.heappush(pend, (g[3], count, k, (0, 0, 0)))
        count += 1
    while pend or ready or any(left) or held:
        while pend and pend[0][0] <= now:
            at, _, k, d = heapq.heappop(pend)
            name, salt, _, _, rank, jump = GROUPS[k]
            heapq.heappush(ready, ((rank, -height(name, d, salt, jump), at), k, d))
        if ready:
            _, k, d = heapq.heappop(ready)
            name, salt, units, _, _, jump = GROUPS[k]
            kids = sorted(children(name, d, salt, jump), key=lambda c: -height(name, c[2], salt, jump))
            log.append(("relay", k, d, kids))
            now += 0.016
            for axis, s, nd in kids:
                now += 0.016
                way = (axis, s > 0)
                busy = units * 4096 / 46.7e3
                start = max(now, free.get(way, 0.0))
                free[way] = start + abs(s) * busy
                heapq.heappush(pend, (start + busy + LATENCY + 0.8 * (abs(s) - 1), count, k, nd))
                count += 1
            got[k] += 1
            if got[k] == NY * NX * NZ:
                done[k] = now + 1.6
            continue
        open_groups = [k for k in range(len(GROUPS)) if left[k] and done[k] is not None]
        best = min(open_groups, key=lambda k: done[k], default=None)
        if best is not None and done[best] <= now:
            log.append(("unit", best, GROUPS[best][2] - left[best]))
            left[best] -= 1
            now += 0.7 if held else 0.4
            held = True
            continue
        later = min([p[0] for p in pend[:1]] + [done[k] for k in open_groups], default=now + 9)
        if held and later > now + 0.3:
            log.append(("flush",))
            now += 0.55
            held = False
            continue
        now = later
    return log


def score(q, buf, unit, kk, scores):
    keys = SLOTS * ROWS
    kk[...] = buf[:, 2 * unit].astype(jnp.float32).reshape(keys, HD).astype(jnp.bfloat16)
    for at in range(0, keys, 256):
        scores[:, at : at + 256] = lax.dot_general(
            q, kk[at : at + 256], (((1,), (1,)), ((), ())), preferred_element_type=jnp.float32
        )


def mix(buf, unit, vv, scores, block):
    vv[:, :HD] = buf[:, 2 * unit + 1].astype(jnp.float32).reshape(SLOTS * ROWS, HD).astype(jnp.bfloat16)
    outs = []
    for r in range(0, scores.shape[0], block):
        part = scores[r : r + block]
        part = (part - jnp.max(part, axis=1, keepdims=True)) * (LOG2E / HD**0.5)
        expo = jnp.exp2(part).astype(jnp.bfloat16)
        mixed = jnp.dot(expo, vv[...], preferred_element_type=jnp.float32)
        outs.append(mixed[:, :HD] / mixed[:, HD:])
    return outs


def kernel(
    qs_hbm, kvs_hbm, qt_hbm, kvt_hbm, outs, outt, loss_ref,
    buf, qs, qt, kk, vv, scores, other, acc,
    total_in, total_out, load_sem, q_sem, ici_send, d2d_send, ici_recv, d2d_recv, sum_send, sum_recv,
):
    seq = lax.axis_index("seq")
    dp = lax.axis_index("dp")
    core = lax.rem(seq, 2)
    z = lax.rem(seq // 2, NZ)
    x = lax.rem(seq // (2 * NZ), NX)
    y = seq // (2 * NZ * NX)

    def device(yy, xx, zz, cc, dd=dp):
        return {"seq": ((yy * NX + xx) * NZ + zz) * 2 + cc, "dp": dd}

    def line(cc, yy, xx):
        return ((cc * NY + yy) * NX + xx) * NZ

    near = {
        ("z", 1): device(y, x, lax.rem(z + 1, NZ), core),
        ("z", -1): device(y, x, lax.rem(z + NZ - 1, NZ), core),
        ("z", 2): device(y, x, lax.rem(z + 2, NZ), core),
        ("z", -2): device(y, x, lax.rem(z + NZ - 2, NZ), core),
        ("y", 1): device(lax.rem(y + 1, NY), x, z, core),
        ("y", -1): device(lax.rem(y + NY - 1, NY), x, z, core),
        ("y", 2): device(lax.rem(y + 2, NY), x, z, core),
        ("y", -2): device(lax.rem(y + 2, NY), x, z, core),
        ("x", 1): device(y, 1 - x, z, core),
    }
    partner = device(y, x, z, 1 - core)
    ys = [lax.rem(y + NY - d, NY) for d in range(NY)]
    xs = [x, 1 - x]
    zs = [lax.rem(z + NZ - d, NZ) for d in range(NZ)]

    cube = []
    for i in range(1, 8):
        cube.append(device(y, lax.rem(x + i // 4, 2), z, lax.rem(core + i // 2 % 2, 2), lax.rem(dp + i % 2, 2)))
    plane = [
        device(lax.rem(y + i // NZ, NY), x, lax.rem(z + i % NZ, NZ), core) for i in range(1, NY * NZ)
    ]
    sums = ((y * NZ + z, plane), ((x * 2 + core) * 2 + dp, cube))
    peers = [to for way, to in near.items() if way not in (("y", -2), ("x", 1))] + cube

    mine = line(core, y, x) + z
    barrier = pltpu.get_barrier_semaphore()
    for peer in peers:
        pl.semaphore_signal(barrier, inc=1, device_id=peer, device_id_type=pl.DeviceIdType.MESH)
    for unit in range(UNITS):
        head, kv = unit // 2, (kvs_hbm, kvt_hbm)[unit % 2]
        for part in range(2):
            cols = pl.ds(part * WIDTH + head * HD, HD)
            pltpu.make_async_copy(kv.at[0, :, cols], buf.at[mine, 2 * unit + part], load_sem.at[0]).start()
    load_q = [
        pltpu.make_async_copy(qs_hbm.at[0], qs, q_sem.at[0]),
        pltpu.make_async_copy(qt_hbm.at[0], qt, q_sem.at[1]),
    ]
    for c in load_q:
        c.start()
    vv[:, :, HD:] = jnp.ones((KEEP, SLOTS * ROWS, HD), jnp.bfloat16)
    acc[...] = jnp.zeros_like(acc)
    pltpu.make_async_copy(buf.at[mine], buf.at[mine], load_sem.at[0]).wait()
    pl.semaphore_wait(barrier, len(peers))

    def remote(part, send, recv, to):
        return pltpu.make_async_remote_copy(
            src_ref=part, dst_ref=part, send_sem=send, recv_sem=recv,
            device_id=to, device_id_type=pl.DeviceIdType.MESH,
        )

    def cut(k):
        return pl.ds(2 * FIRST[k], 2 * GROUPS[k][2])

    def item(k, d):
        return buf.at[line(core, ys[d[0]], xs[d[1]]) + zs[d[2]], cut(k)]

    def sem_of(k, d):
        return ici_recv.at[k, (d[0] * NX + d[1]) * NZ + d[2]]

    rows = qs.shape[0]
    block = 256
    have, ran, seen, loaded = {}, 0, set(), False

    def finish(unit, slot):
        head, model = unit // 2, unit % 2
        cols = slice(head * HD, head * HD + HD)
        for i, r in enumerate(mix(buf, unit, vv.at[slot], scores.at[slot], block)):
            at = slice(i * block, i * block + block)
            (outs, outt)[model][0, at, cols] = r.astype(jnp.bfloat16)
            if head in seen:
                gap = other[head, at, :] - r
                acc[at, :] += gap * gap
            else:
                other[head, at, :] = r
        seen.add(head)

    held = None
    for kind, *what in plan():
        if kind == "flush":
            finish(*held)
            held = None
            continue
        if kind == "unit":
            k, d = what
            if not loaded:
                for c in load_q:
                    c.wait()
                loaded = True
            if d == 0:
                part = buf.at[pl.ds((1 - core) * LINES * NZ, LINES * NZ), cut(k)]
                remote(part, d2d_send.at[k], d2d_recv.at[k], partner).wait_recv()
            unit = FIRST[k] + d
            slot = ran % KEEP
            ran += 1
            score((qs, qt)[unit % 2][:, unit // 2 * HD : unit // 2 * HD + HD], buf, unit, kk.at[slot], scores.at[slot])
            if held:
                finish(*held)
            held = (unit, slot)
            continue
        k, d, kids = what
        if d != (0, 0, 0):
            remote(item(k, d), ici_send.at[k], sem_of(k, d), partner).wait_recv()
        for axis, s, nd in kids:
            remote(item(k, d), ici_send.at[k], sem_of(k, nd), near[(axis, s)]).start()
        spot = (k, d[0], d[1])
        have[spot] = have.get(spot, 0) + 1
        if have[spot] == NZ:
            part = buf.at[pl.ds(line(core, ys[d[0]], xs[d[1]]), NZ), cut(k)]
            remote(part, d2d_send.at[k], d2d_recv.at[k], partner).start()

    spot = lax.broadcasted_iota(jnp.int32, (rows, HD), 0) + ((y * NX + x) * NZ + z) * 2 * rows + core * rows
    weight = 1.0 + 2.0 * spot.astype(jnp.float32) / float(rows * SLOTS - 1)
    total = jnp.sum(weight * acc[...], axis=0, keepdims=True)
    for i, (spot, group) in enumerate(sums):
        total_out[i] = total
        total_in[i, spot] = total
        for to in group:
            pltpu.make_async_remote_copy(
                src_ref=total_out.at[i], dst_ref=total_in.at[i, spot], send_sem=sum_send.at[i],
                recv_sem=sum_recv.at[i], device_id=to, device_id_type=pl.DeviceIdType.MESH,
            ).start()
        every = total_in.at[i, pl.ds(0, len(group))]
        remote(every, sum_send.at[i], sum_recv.at[i], partner).wait()
        total = jnp.sum(total_in[i, : len(group) + 1], axis=0)
    loss_ref[...] = total

    for k in range(len(GROUPS)):
        part = buf.at[pl.ds(0, LINES * NZ - 1), cut(k)]
        remote(part, ici_send.at[k], d2d_recv.at[k], partner).wait_send()
        part = buf.at[pl.ds(0, LINES * NZ), cut(k)]
        remote(part, d2d_send.at[k], d2d_recv.at[k], partner).wait_send()


def write(count, s_ref, t_ref, total_ref, os_hbm, ot_hbm, loss_ref, sem):
    copies = [
        pltpu.make_async_copy(s_ref, os_hbm, sem.at[0]),
        pltpu.make_async_copy(t_ref, ot_hbm, sem.at[1]),
    ]
    for c in copies:
        c.start()
    loss_ref[0] = jnp.sum(total_ref[...]) / count
    for c in copies:
        c.wait()


def body(q_student, kv_student, q_target, kv_target):
    rows = q_student.shape[1]
    bf = jnp.bfloat16
    any_space = pl.BlockSpec(memory_space=pl.ANY)
    vmem = pl.BlockSpec(memory_space=pltpu.VMEM)
    student, target, total = pl.pallas_call(
        kernel,
        out_shape=(
            pltpu.VMEM(q_student.shape, bf),
            pltpu.VMEM(q_student.shape, bf),
            pltpu.VMEM((1, HD), jnp.float32),
        ),
        in_specs=[any_space] * 4,
        out_specs=(vmem,) * 3,
        scratch_shapes=[
            pltpu.VMEM((SLOTS, 2 * UNITS, ROWS, HD), bf),
            pltpu.VMEM((rows, WIDTH), bf),
            pltpu.VMEM((rows, WIDTH), bf),
            pltpu.VMEM((KEEP, SLOTS * ROWS, HD), bf),
            pltpu.VMEM((KEEP, SLOTS * ROWS, 2 * HD), bf),
            pltpu.VMEM((KEEP, rows, SLOTS * ROWS), jnp.float32),
            pltpu.VMEM((HEADS, rows, HD), jnp.float32),
            pltpu.VMEM((rows, HD), jnp.float32),
            pltpu.VMEM((2, NY * NZ, 1, HD), jnp.float32),
            pltpu.VMEM((2, 1, HD), jnp.float32),
            pltpu.SemaphoreType.DMA((1,)),
            pltpu.SemaphoreType.DMA((2,)),
            pltpu.SemaphoreType.DMA((len(GROUPS),)),
            pltpu.SemaphoreType.DMA((len(GROUPS),)),
            pltpu.SemaphoreType.DMA((len(GROUPS), LINES * NZ)),
            pltpu.SemaphoreType.DMA((len(GROUPS),)),
            pltpu.SemaphoreType.DMA((2,)),
            pltpu.SemaphoreType.DMA((2,)),
        ],
        compiler_params=pltpu.CompilerParams(
            collective_id=0, has_side_effects=True, vmem_limit_bytes=52 * 1024 * 1024
        ),
    )(q_student, kv_student, q_target, kv_target)
    student, target, loss = pl.pallas_call(
        functools.partial(write, float(rows * SLOTS * WIDTH)),
        out_shape=(
            jax.ShapeDtypeStruct(q_student.shape, bf),
            jax.ShapeDtypeStruct(q_student.shape, bf),
            jax.ShapeDtypeStruct((1,), jnp.float32),
        ),
        in_specs=[vmem] * 3,
        out_specs=(any_space, any_space, pl.BlockSpec(memory_space=pltpu.SMEM)),
        scratch_shapes=[pltpu.SemaphoreType.DMA((2,))],
        compiler_params=pltpu.CompilerParams(vmem_limit_bytes=16 * 1024 * 1024),
    )(student, target, total)
    return student, target, loss.reshape(())


def solution(mesh):
    spec = P("dp", "seq", None)
    return jax.shard_map(
        body, mesh=mesh, in_specs=(spec,) * 4, out_specs=(spec, spec, P()), check_vma=False
    )
```
